32 devices in a mesh: xy: 16 (over z, y, core), gz: 2 (over x).
Axes of the slice: x: 2, y: 2, z: 4, core: 2. Of those that a mesh axis runs over, the one named last changes fastest.
Arguments:
- e_check: float32 [3, 128, 4, 1024], P(None, 'xy', 'gz'), may hold values from -6 to 6
- h_check: float32 [3, 128, 4, 1024], P(None, 'xy', 'gz'), may hold values from -6 to 6
- adj_e: float32 [3, 128, 4, 1024], P(None, 'xy', 'gz'), may hold values from -6 to 6
- adj_h: float32 [3, 128, 4, 1024], P(None, 'xy', 'gz'), may hold values from -6 to 6
- material: int32 [128, 4, 1024], P('xy', 'gz'), may hold values from 0 to 3
- owner: int32 [128, 4, 1024], P('xy', 'gz'), may hold values from 0 to 7
- permittivity: float32 [4], replicated, may hold values from 1 to 4
Outputs:
- adj_e_out: float32 [3, 128, 4, 1024], P(None, 'xy', 'gz')
- adj_h_out: float32 [3, 128, 4, 1024], P(None, 'xy', 'gz')
- height_grad: float32 [8], replicated
The draws below stay inside these ranges and needn't reach their ends.
All inputs are finite; a program needn't handle non-finite values.
Results may differ from the reference program's by a relative error of at most 0.0003.
Values sent between devices are 32-bit elements; how exact they have to be, the bound alone decides.
A program may use at most 64 MiB of HBM per device.

```python
import math
import jax
import jax.numpy as jnp
from jax import lax

NY = 1024
NI = 8
NX = 128
NZ = 4


def plant(entries, own_key, least, top_value):
    spot = [jax.random.randint(jax.random.fold_in(own_key, axis), (), 0, length) for axis, length in enumerate(entries.shape)]
    longest = entries.shape.index(max(entries.shape))
    neighbour = spot[:longest] + [(spot[longest] + 1) % entries.shape[longest]] + spot[longest + 1:]
    return entries.at[tuple(spot)].set(least).at[tuple(neighbour)].set(top_value)


def block_scale(rng, extent, split, least, largest):
    factor_of, own = 1.0, jax.random.fold_in(rng, 6)
    for dim, blocks in split:
        steps = jnp.exp(jax.random.uniform(jax.random.fold_in(own, dim), (blocks,), jnp.float32, least / len(split), largest / len(split)))
        factor_of = factor_of * jnp.repeat(steps, extent[dim] // blocks).reshape([-1 if axis == dim else 1 for axis in range(len(extent))])
    return factor_of


def centred(key, shape, scale, limit, shards=(), dtype=jnp.bfloat16):
    gain = block_scale(key, shape, shards, -0.22, 0.18) if shards else 1.0
    drawn = jax.random.normal(key, shape, jnp.float32) * scale * gain
    return jnp.minimum(jnp.maximum(drawn, -limit), limit).astype(dtype)


def setup_inputs(seed: int = 0) -> dict:
    splits = jax.random.split(jax.random.key(seed), 8)
    return {
        "e_check": centred(splits[0], (3, NX, NZ, NY), 1.0, 6.0, ((1, 16), (2, 2)), jnp.float32),
        "h_check": centred(splits[1], (3, NX, NZ, NY), 1.0, 6.0, ((1, 16), (2, 2)), jnp.float32),
        "adj_e": centred(splits[2], (3, NX, NZ, NY), 1.0, 6.0, ((1, 16), (2, 2)), jnp.float32),
        "adj_h": centred(splits[3], (3, NX, NZ, NY), 1.0, 6.0, ((1, 16), (2, 2)), jnp.float32),
        "material": plant(jax.random.randint(splits[4], (NX, NZ, NY), 0, 4), jax.random.fold_in(splits[4], 1), 0, 3).astype(jnp.int32),
        "owner": plant(jax.random.randint(splits[5], (NX, NZ, NY), 0, NI), jax.random.fold_in(splits[5], 1), 0, NI - 1).astype(jnp.int32),
        "permittivity": jnp.clip(jnp.exp(jax.random.uniform(splits[6], (4,), jnp.float32, math.log(1.0), math.log(4.0))), 1.0, 4.0),
    }


COURANT = 0.5

def diff_ahead(values, dim_axis):
    count = values.shape[dim_axis]
    zero_plane = jnp.zeros_like(lax.slice_in_dim(values, 0, 1, axis=dim_axis))
    later = jnp.concatenate([lax.slice_in_dim(values, 1, count, axis=dim_axis), zero_plane], axis=dim_axis)
    return later - values

def diff_behind(values, dim_axis):
    count = values.shape[dim_axis]
    zero_plane = jnp.zeros_like(lax.slice_in_dim(values, 0, 1, axis=dim_axis))
    earlier = jnp.concatenate([zero_plane, lax.slice_in_dim(values, 0, count - 1, axis=dim_axis)], axis=dim_axis)
    return values - earlier

def curl_with(fields, differ):
    comp_x, comp_y, comp_z = (fields[0], fields[1], fields[2])
    curl_x = differ(comp_z, 2) - differ(comp_y, 1)
    curl_y = differ(comp_x, 1) - differ(comp_z, 0)
    curl_z = differ(comp_y, 0) - differ(comp_x, 2)
    return jnp.stack([curl_x, curl_y, curl_z], axis=0)

def reference(e_check, h_check, adj_e, adj_h, material, owner, permittivity):
    e_coef = COURANT / permittivity[material]
    electric = [e_check]
    magnetic = h_check
    for index_step in range(2):
        magnetic = magnetic - COURANT * curl_with(electric[-1], diff_ahead)
        electric.append(electric[-1] + e_coef * curl_with(magnetic, diff_behind))
    adjoint_e, adjoint_h = (adj_e, adj_h)
    gradient = jnp.zeros((NI,), jnp.float32)
    for later_step in (2, 1):
        weight = e_coef * lax.optimization_barrier(jnp.sum(adjoint_e * (electric[later_step] - electric[later_step - 1]), axis=0))
        gradient = gradient + jax.ops.segment_sum(weight.reshape(-1), owner.reshape(-1).astype(jnp.int32), num_segments=NI)
        adjoint_h = adjoint_h + curl_with(e_coef * adjoint_e, diff_ahead)
        adjoint_e = adjoint_e - COURANT * curl_with(adjoint_h, diff_behind)
    total_cells = NX * NZ * NY
    gradient = gradient / jnp.sqrt(jnp.float32(total_cells / NI))
    return (adjoint_e, adjoint_h, gradient)
```

```python
import functools

import jax
import jax.numpy as jnp
import numpy as np
from jax import lax
from jax.experimental import pallas as pl
from jax.experimental.pallas import tpu as pltpu
from jax.sharding import PartitionSpec as P

NI = 8
COURANT = 0.5
MESH = pl.DeviceIdType.MESH
SCALES = (-COURANT, 1.0)


def kernel(
    dims, e_hbm, h_hbm, g_hbm, k_hbm, mat_hbm, own_hbm, perm,
    go_hbm, ko_hbm, grad_ref,
    field, inner, partial, curl_in, outer, mat, own, coef, weight,
    send_xf, send_xl, send_d5, send_d6,
    got_xf, got_zf, got_xl, got_zl, got_d5, got_d6,
    mine, gathered,
    load_sem, send_sem, recv_sem, sum_send, sum_recv, out_sem,
):
    n_x, n_z, nx, nz, ny, kinds, norm = dims
    total = n_x * n_z
    i = lax.axis_index("xy")
    k = lax.axis_index("gz")
    me = i * n_z + k

    def load(src, dst, slot):
        copies = []
        for z in range(nz):
            src_z = src.at[:, :, z, :] if len(src.shape) == 4 else src.at[:, z, :]
            dst_z = dst.at[:, z] if len(src.shape) == 4 else dst.at[z]
            copies.append(pltpu.make_async_copy(src_z, dst_z, load_sem.at[slot, z]))
        return copies

    loads = [
        load(e_hbm, field.at[0], 0),
        load(h_hbm, inner.at[0], 1),
        load(mat_hbm, mat, 2),
        load(g_hbm, outer, 3),
        load(k_hbm, inner.at[1], 4),
        load(own_hbm, own, 5),
    ]
    for group in loads:
        for copy in group:
            copy.start()

    barrier = pltpu.get_barrier_semaphore()

    def greet(step, carry):
        other = lax.rem(me + step, total)
        pl.semaphore_signal(
            barrier, inc=1, device_id=(other // n_z, lax.rem(other, n_z)), device_id_type=MESH
        )
        return carry

    lax.fori_loop(1, total, greet, 0)

    rows = lax.broadcasted_iota(jnp.int32, (nx, ny), 0)
    lanes = lax.broadcasted_iota(jnp.int32, (nx, ny), 1)
    first_row, last_row = rows == 0, rows == nx - 1
    first_lane, last_lane = lanes == 0, lanes == ny - 1

    def dy(v):
        return jnp.where(last_lane, 0.0, pltpu.roll(v, ny - 1, 1)) - v

    def dx(v):
        return jnp.where(last_row, 0.0, pltpu.roll(v, nx - 1, 0)) - v

    def by(v):
        return v - jnp.where(first_lane, 0.0, pltpu.roll(v, 1, 1))

    def bx(v, row):
        return v - jnp.where(first_row, row, pltpu.roll(v, 1, 0))

    def local_part(q, mag):
        scale = SCALES[q % 2]
        f = field.at[q]
        for z in range(nz):
            fx, fy, fz = f[0, z], f[1, z], f[2, z]
            if z < nz - 1:
                up_x, up_y = f[0, z + 1] - fx, f[1, z + 1] - fy
            else:
                up_x, up_y = -fx, -fy
            lx = mag[0, z] + scale * (dy(fz) - up_y)
            ly = mag[1, z] + scale * (up_x - dx(fz))
            lz = mag[2, z] + scale * (dx(fy) - dy(fx))
            partial[q, 0, z], partial[q, 1, z], partial[q, 2, z] = lx, ly, lz
            send_xf[q, z : z + 1] = fy[0:1]
            send_xf[q, nz + z : nz + z + 1] = fz[0:1]
            send_xl[q, z : z + 1] = ly[nx - 1 : nx]
            send_xl[q, nz + z : nz + z + 1] = lz[nx - 1 : nx]
            if z == 0:
                send_d5[q] = fx[nx - 1 : nx]
            if z == nz - 1:
                send_d6[q] = fz[0:1]

    def messages(q):
        below_x, above_x = i > 0, i < n_x - 1
        below_z, above_z = k > 0, k < n_z - 1
        table = (
            (field.at[q, 0:2, 0], got_zf.at[q], (i, k - 1), below_z, above_z),
            (partial.at[q, 0:2, nz - 1], got_zl.at[q], (i, k + 1), above_z, below_z),
            (send_xf.at[q], got_xf.at[q], (i - 1, k), below_x, above_x),
            (send_xl.at[q], got_xl.at[q], (i + 1, k), above_x, below_x),
            (send_d5.at[q], got_d5.at[q], (i + 1, k - 1), above_x & below_z, below_x & above_z),
            (send_d6.at[q], got_d6.at[q], (i - 1, k + 1), below_x & above_z, above_x & below_z),
        )
        return [
            (
                pltpu.make_async_remote_copy(
                    src_ref=src, dst_ref=dst, send_sem=send_sem.at[q, m],
                    recv_sem=recv_sem.at[q, m], device_id=target, device_id_type=MESH,
                ),
                sends,
                receives,
            )
            for m, (src, dst, target, sends, receives) in enumerate(table)
        ]

    def send(q):
        for copy, sends, _ in messages(q):
            pl.when(sends)(copy.start)

    def receive(q):
        for copy, _, receives in messages(q):
            pl.when(receives)(copy.wait_recv)

    def finish(q, put):
        scale = SCALES[q % 2]
        f, part = field.at[q], partial.at[q]
        not_first_x, not_last_x = i > 0, i < n_x - 1
        not_first_z, not_last_z = k > 0, k < n_z - 1

        def only(cond, v):
            return jnp.where(cond, v, 0.0)

        below_x = only(not_first_z, got_zl[q, 0] - scale * f[1, 0])
        below_y = got_zl[q, 1] + scale * f[0, 0]
        diagonal = only(not_last_x, scale * got_d6[q])
        below_y = only(not_first_z, below_y - jnp.where(last_row, diagonal, 0.0))
        result = []
        for z in range(nz):
            mx, my, mz = part[0, z], part[1, z], part[2, z]
            edge_y = got_xl[q, z : z + 1] - scale * f[2, z, 0:1]
            edge_z = got_xl[q, nz + z : nz + z + 1] + scale * f[1, z, 0:1]
            if z == nz - 1:
                mx = mx - only(not_last_z, scale * got_zf[q, 1])
                my = my + only(not_last_z, scale * got_zf[q, 0])
                edge_y = edge_y + only(not_last_z, scale * got_d5[q])
            edge_y, edge_z = only(not_first_x, edge_y), only(not_first_x, edge_z)
            next_y = only(not_last_x, scale * got_xf[q, z : z + 1])
            next_z = only(not_last_x, scale * got_xf[q, nz + z : nz + z + 1])
            my = my - jnp.where(last_row, next_z, 0.0)
            mz = mz + jnp.where(last_row, next_y, 0.0)
            if put is not None:
                put[0, z], put[1, z], put[2, z] = mx, my, mz
            result.append(
                (
                    by(mz) - (my - below_y),
                    (mx - below_x) - bx(mz, edge_z),
                    bx(my, edge_y) - by(mx),
                )
            )
            below_x, below_y = mx, my
        return result

    for slot in (0, 1):
        for copy in loads[slot]:
            copy.wait()
    local_part(0, inner.at[0])
    for slot in (2, 3, 4):
        for copy in loads[slot]:
            copy.wait()
    for z in range(nz):
        kind = mat[z]
        eps = jnp.full((nx, ny), perm[0], jnp.float32)
        for number in range(1, kinds):
            eps = jnp.where(kind == number, perm[number], eps)
        coef[z] = COURANT / eps
        for c in range(3):
            field[1, c, z] = coef[z] * outer[c, z]
    pl.semaphore_wait(barrier, total - 1)
    send(0)
    local_part(1, inner.at[1])
    send(1)

    receive(0)
    change = finish(0, curl_in.at[0])
    for z in range(nz):
        for c in range(3):
            moved = coef[z] * change[z][c]
            curl_in[2, c, z] = moved
            field[2, c, z] = field[0, c, z] + moved
    local_part(2, curl_in.at[0])
    send(2)

    receive(1)
    change = finish(1, curl_in.at[1])
    for z in range(nz):
        dot = None
        for c in range(3):
            now = outer[c, z] - COURANT * change[z][c]
            inner[1, c, z] = now
            field[3, c, z] = coef[z] * now
            term = now * curl_in[2, c, z]
            dot = term if dot is None else dot + term
        weight[z] = coef[z] * dot
    local_part(3, curl_in.at[1])
    send(3)
    for copy in loads[5]:
        copy.wait()

    receive(2)
    change = finish(2, None)
    sums = [None] * NI
    for z in range(nz):
        dot = None
        for c in range(3):
            term = outer[c, z] * (coef[z] * change[z][c])
            dot = term if dot is None else dot + term
        both = weight[z] + coef[z] * dot
        which = own[z]
        for j in range(NI):
            share = jnp.sum(jnp.where(which == j, both, 0.0), axis=0, keepdims=True)
            sums[j] = share if sums[j] is None else sums[j] + share
    lane = lax.broadcasted_iota(jnp.int32, (1, 128), 1)
    line = jnp.zeros((1, 128), jnp.float32)
    for j in range(NI):
        line = jnp.where(lane == j, jnp.sum(sums[j], axis=1, keepdims=True), line)
    mine[0] = line
    gathered[me] = line

    def share_sum(step, carry):
        other = lax.rem(me + step, total)
        pltpu.make_async_remote_copy(
            src_ref=mine.at[0], dst_ref=gathered.at[me], send_sem=sum_send, recv_sem=sum_recv,
            device_id=(other // n_z, lax.rem(other, n_z)), device_id_type=MESH,
        ).start()
        return carry

    lax.fori_loop(1, total, share_sum, 0)

    receive(3)
    change = finish(3, inner.at[0])
    for z in range(nz):
        for c in range(3):
            outer[c, z] = inner[1, c, z] - COURANT * change[z][c]
    outs = []
    for z in range(nz):
        outs.append(pltpu.make_async_copy(inner.at[0, :, z], ko_hbm.at[:, :, z, :], out_sem.at[0, z]))
        outs.append(pltpu.make_async_copy(outer.at[:, z], go_hbm.at[:, :, z, :], out_sem.at[1, z]))
    for copy in outs:
        copy.start()

    everyone = gathered.at[0 : total - 1]
    pltpu.make_async_copy(everyone, everyone, sum_recv).wait()
    pltpu.make_async_copy(everyone, everyone, sum_send).wait()
    grad_ref[...] = jnp.sum(gathered[...], axis=0)[:, :NI] / norm
    for q in range(4):
        for copy, sends, _ in messages(q):
            pl.when(sends)(copy.wait_send)
    for copy in outs:
        copy.wait()


def solution(mesh):
    n_x, n_z = mesh.shape["xy"], mesh.shape["gz"]

    def body(e_check, h_check, adj_e, adj_h, material, owner, permittivity):
        _, nx, nz, ny = e_check.shape
        cells = nx * n_x * nz * n_z * ny
        norm = np.sqrt(np.float32(cells / NI))
        dims = (n_x, n_z, nx, nz, ny, permittivity.shape[0], norm)
        f32 = jnp.float32
        any_spec = pl.BlockSpec(memory_space=pl.ANY)
        block = (3, nz, nx, ny)
        g, h, grad = pl.pallas_call(
            functools.partial(kernel, dims),
            out_shape=(
                jax.ShapeDtypeStruct(e_check.shape, f32),
                jax.ShapeDtypeStruct(e_check.shape, f32),
                jax.ShapeDtypeStruct((1, NI), f32),
            ),
            in_specs=[any_spec] * 6 + [pl.BlockSpec(memory_space=pltpu.SMEM)],
            out_specs=(any_spec, any_spec, pl.BlockSpec(memory_space=pltpu.VMEM)),
            scratch_shapes=[
                pltpu.VMEM((4,) + block, f32),
                pltpu.VMEM((2,) + block, f32),
                pltpu.VMEM((4,) + block, f32),
                pltpu.VMEM((3,) + block, f32),
                pltpu.VMEM(block, f32),
                pltpu.VMEM((nz, nx, ny), jnp.int32),
                pltpu.VMEM((nz, nx, ny), jnp.int32),
                pltpu.VMEM((nz, nx, ny), f32),
                pltpu.VMEM((nz, nx, ny), f32),
                pltpu.VMEM((4, 2 * nz, ny), f32),
                pltpu.VMEM((4, 2 * nz, ny), f32),
                pltpu.VMEM((4, 1, ny), f32),
                pltpu.VMEM((4, 1, ny), f32),
                pltpu.VMEM((4, 2 * nz, ny), f32),
                pltpu.VMEM((4, 2, nx, ny), f32),
                pltpu.VMEM((4, 2 * nz, ny), f32),
                pltpu.VMEM((4, 2, nx, ny), f32),
                pltpu.VMEM((4, 1, ny), f32),
                pltpu.VMEM((4, 1, ny), f32),
                pltpu.VMEM((1, 1, 128), f32),
                pltpu.VMEM((n_x * n_z, 1, 128), f32),
                pltpu.SemaphoreType.DMA((6, nz)),
                pltpu.SemaphoreType.DMA((4, 6)),
                pltpu.SemaphoreType.DMA((4, 6)),
                pltpu.SemaphoreType.DMA,
                pltpu.SemaphoreType.DMA,
                pltpu.SemaphoreType.DMA((2, nz)),
            ],
            compiler_params=pltpu.CompilerParams(collective_id=0, has_side_effects=True),
            name="yee_adjoint",
        )(e_check, h_check, adj_e, adj_h, material, owner, permittivity)
        return g, h, grad.reshape(NI)

    split = P(None, "xy", "gz", None)
    return jax.shard_map(
        body,
        mesh=mesh,
        in_specs=(split,) * 4 + (P("xy", "gz", None),) * 2 + (P(),),
        out_specs=(split, split, P()),
        check_vma=False,
    )
```

```python
import functools

import jax
import jax.numpy as jnp
import numpy as np
from jax import lax
from jax.experimental import pallas as pl
from jax.experimental.pallas import tpu as pltpu
from jax.sharding import PartitionSpec as P

NI = 8
COURANT = 0.5
MESH = pl.DeviceIdType.MESH
SCALES = (-COURANT, 1.0)


def kernel(
    dims, e_hbm, h_hbm, g_hbm, k_hbm, mat_hbm, own_hbm, perm,
    go_ref, ko_ref, grad_ref,
    field, inner, partial, curl_in, outer, mat, own, coef, weight,
    send_xf, send_xl, send_d5, send_d6,
    got_xf, got_zf, got_xl, got_zl, got_d5, got_d6,
    mine, gathered,
    load_sem, send_sem, recv_sem, sum_send, sum_recv,
):
    n_x, n_z, nx, nz, ny, kinds, norm = dims
    total = n_x * n_z
    i = lax.axis_index("xy")
    k = lax.axis_index("gz")
    me = i * n_z + k

    def load(src, dst, slot):
        copies = []
        for z in range(nz):
            src_z = src.at[:, :, z, :] if len(src.shape) == 4 else src.at[:, z, :]
            dst_z = dst.at[:, z] if len(src.shape) == 4 else dst.at[z]
            copies.append(pltpu.make_async_copy(src_z, dst_z, load_sem.at[slot, z]))
        return copies

    loads = [
        load(e_hbm, field.at[0], 0),
        load(h_hbm, inner.at[0], 1),
        load(mat_hbm, mat, 2),
        load(g_hbm, outer, 3),
        load(k_hbm, inner.at[1], 4),
        load(own_hbm, own, 5),
    ]
    for group in loads:
        for copy in group:
            copy.start()

    barrier = pltpu.get_barrier_semaphore()

    def greet(step, carry):
        other = lax.rem(me + step, total)
        pl.semaphore_signal(
            barrier, inc=1, device_id=(other // n_z, lax.rem(other, n_z)), device_id_type=MESH
        )
        return carry

    lax.fori_loop(1, total, greet, 0)

    rows = lax.broadcasted_iota(jnp.int32, (nx, ny), 0)
    lanes = lax.broadcasted_iota(jnp.int32, (nx, ny), 1)
    first_row, last_row = rows == 0, rows == nx - 1
    first_lane, last_lane = lanes == 0, lanes == ny - 1

    def dy(v):
        return jnp.where(last_lane, 0.0, pltpu.roll(v, ny - 1, 1)) - v

    def dx(v):
        return jnp.where(last_row, 0.0, pltpu.roll(v, nx - 1, 0)) - v

    def by(v):
        return v - jnp.where(first_lane, 0.0, pltpu.roll(v, 1, 1))

    def bx(v, row):
        return v - jnp.where(first_row, row, pltpu.roll(v, 1, 0))

    def local_part(q, mag):
        scale = SCALES[q % 2]
        f = field.at[q]
        for z in range(nz):
            fx, fy, fz = f[0, z], f[1, z], f[2, z]
            if z < nz - 1:
                up_x, up_y = f[0, z + 1] - fx, f[1, z + 1] - fy
            else:
                up_x, up_y = -fx, -fy
            lx = mag[0, z] + scale * (dy(fz) - up_y)
            ly = mag[1, z] + scale * (up_x - dx(fz))
            lz = mag[2, z] + scale * (dx(fy) - dy(fx))
            partial[q, 0, z], partial[q, 1, z], partial[q, 2, z] = lx, ly, lz
            send_xf[q, z : z + 1] = fy[0:1]
            send_xf[q, nz + z : nz + z + 1] = fz[0:1]
            send_xl[q, z : z + 1] = ly[nx - 1 : nx]
            send_xl[q, nz + z : nz + z + 1] = lz[nx - 1 : nx]
            if z == 0:
                send_d5[q] = fx[nx - 1 : nx]
            if z == nz - 1:
                send_d6[q] = fz[0:1]

    def messages(q):
        below_x, above_x = i > 0, i < n_x - 1
        below_z, above_z = k > 0, k < n_z - 1
        table = (
            (send_d5.at[q], got_d5.at[q], (i + 1, k - 1), above_x & below_z, below_x & above_z),
            (send_d6.at[q], got_d6.at[q], (i - 1, k + 1), below_x & above_z, above_x & below_z),
            (send_xf.at[q], got_xf.at[q], (i - 1, k), below_x, above_x),
            (send_xl.at[q], got_xl.at[q], (i + 1, k), above_x, below_x),
            (field.at[q, 0:2, 0], got_zf.at[q], (i, k - 1), below_z, above_z),
            (partial.at[q, 0:2, nz - 1], got_zl.at[q], (i, k + 1), above_z, below_z),
        )
        return [
            (
                pltpu.make_async_remote_copy(
                    src_ref=src, dst_ref=dst, send_sem=send_sem.at[q, m],
                    recv_sem=recv_sem.at[q, m], device_id=target, device_id_type=MESH,
                ),
                sends,
                receives,
            )
            for m, (src, dst, target, sends, receives) in enumerate(table)
        ]

    def send(q):
        for copy, sends, _ in messages(q):
            pl.when(sends)(copy.start)

    def receive(q):
        for copy, _, receives in messages(q):
            pl.when(receives)(copy.wait_recv)

    def finish(q, put):
        scale = SCALES[q % 2]
        f, part = field.at[q], partial.at[q]
        not_first_x, not_last_x = i > 0, i < n_x - 1
        not_first_z, not_last_z = k > 0, k < n_z - 1

        def only(cond, v):
            return jnp.where(cond, v, 0.0)

        below_x = only(not_first_z, got_zl[q, 0] - scale * f[1, 0])
        below_y = got_zl[q, 1] + scale * f[0, 0]
        diagonal = only(not_last_x, scale * got_d6[q])
        below_y = only(not_first_z, below_y - jnp.where(last_row, diagonal, 0.0))
        result = []
        for z in range(nz):
            mx, my, mz = part[0, z], part[1, z], part[2, z]
            edge_y = got_xl[q, z : z + 1] - scale * f[2, z, 0:1]
            edge_z = got_xl[q, nz + z : nz + z + 1] + scale * f[1, z, 0:1]
            if z == nz - 1:
                mx = mx - only(not_last_z, scale * got_zf[q, 1])
                my = my + only(not_last_z, scale * got_zf[q, 0])
                edge_y = edge_y + only(not_last_z, scale * got_d5[q])
            edge_y, edge_z = only(not_first_x, edge_y), only(not_first_x, edge_z)
            next_y = only(not_last_x, scale * got_xf[q, z : z + 1])
            next_z = only(not_last_x, scale * got_xf[q, nz + z : nz + z + 1])
            my = my - jnp.where(last_row, next_z, 0.0)
            mz = mz + jnp.where(last_row, next_y, 0.0)
            if put is not None:
                put[0, z], put[1, z], put[2, z] = mx, my, mz
            result.append(
                (
                    by(mz) - (my - below_y),
                    (mx - below_x) - bx(mz, edge_z),
                    bx(my, edge_y) - by(mx),
                )
            )
            below_x, below_y = mx, my
        return result

    for slot in (0, 1):
        for copy in loads[slot]:
            copy.wait()
    local_part(0, inner.at[0])
    for slot in (2, 3, 4):
        for copy in loads[slot]:
            copy.wait()
    for z in range(nz):
        kind = mat[z]
        eps = jnp.full((nx, ny), perm[0], jnp.float32)
        for number in range(1, kinds):
            eps = jnp.where(kind == number, perm[number], eps)
        coef[z] = COURANT / eps
        for c in range(3):
            field[1, c, z] = coef[z] * outer[c, z]
    pl.semaphore_wait(barrier, total - 1)
    send(0)
    local_part(1, inner.at[1])
    send(1)

    receive(0)
    change = finish(0, curl_in.at[0])
    for z in range(nz):
        for c in range(3):
            moved = coef[z] * change[z][c]
            curl_in[2, c, z] = moved
            field[2, c, z] = field[0, c, z] + moved
    local_part(2, curl_in.at[0])
    send(2)

    receive(1)
    change = finish(1, curl_in.at[1])
    for z in range(nz):
        dot = None
        for c in range(3):
            now = outer[c, z] - COURANT * change[z][c]
            inner[1, c, z] = now
            field[3, c, z] = coef[z] * now
            term = now * curl_in[2, c, z]
            dot = term if dot is None else dot + term
        weight[z] = coef[z] * dot
    local_part(3, curl_in.at[1])
    send(3)
    for copy in loads[5]:
        copy.wait()

    receive(2)
    change = finish(2, None)
    sums = [jnp.zeros((nx, 128), jnp.float32)] * NI
    for z in range(nz):
        dot = None
        for c in range(3):
            term = outer[c, z] * (coef[z] * change[z][c])
            dot = term if dot is None else dot + term
        both = weight[z] + coef[z] * dot
        which = own[z]
        for t in range(0, ny, 128):
            part, index = both[:, t : t + 128], which[:, t : t + 128]
            for j in range(NI):
                sums[j] = sums[j] + jnp.where(index == j, part, 0.0)
    lane = lax.broadcasted_iota(jnp.int32, (1, 128), 1)
    line = jnp.zeros((1, 128), jnp.float32)
    for j in range(NI):
        column = jnp.sum(sums[j], axis=0, keepdims=True)
        line = jnp.where(lane == j, jnp.sum(column, axis=1, keepdims=True), line)
    mine[0] = line
    gathered[me] = line

    def share_sum(step, carry):
        other = lax.rem(me + step, total)
        pltpu.make_async_remote_copy(
            src_ref=mine.at[0], dst_ref=gathered.at[me], send_sem=sum_send, recv_sem=sum_recv,
            device_id=(other // n_z, lax.rem(other, n_z)), device_id_type=MESH,
        ).start()
        return carry

    lax.fori_loop(1, total, share_sum, 0)

    receive(3)
    change = finish(3, ko_ref)
    for z in range(nz):
        for c in range(3):
            go_ref[c, z] = inner[1, c, z] - COURANT * change[z][c]
    everyone = gathered.at[0 : total - 1]
    pltpu.make_async_copy(everyone, everyone, sum_recv).wait()
    pltpu.make_async_copy(everyone, everyone, sum_send).wait()
    grad_ref[...] = jnp.sum(gathered[...], axis=0)[:, :NI] / norm
    for q in range(4):
        for copy, sends, _ in messages(q):
            pl.when(sends)(copy.wait_send)

def store(g_ref, h_ref, grad_ref, g_hbm, h_hbm, grad_hbm, sem):
    copies = [pltpu.make_async_copy(grad_ref, grad_hbm, sem.at[2, 0])]
    for z in range(g_ref.shape[1]):
        copies.append(pltpu.make_async_copy(g_ref.at[:, z], g_hbm.at[:, :, z, :], sem.at[0, z]))
        copies.append(pltpu.make_async_copy(h_ref.at[:, z], h_hbm.at[:, :, z, :], sem.at[1, z]))
    for copy in copies:
        copy.start()
    for copy in copies:
        copy.wait()


def solution(mesh):
    n_x, n_z = mesh.shape["xy"], mesh.shape["gz"]

    def body(e_check, h_check, adj_e, adj_h, material, owner, permittivity):
        _, nx, nz, ny = e_check.shape
        cells = nx * n_x * nz * n_z * ny
        norm = np.sqrt(np.float32(cells / NI))
        dims = (n_x, n_z, nx, nz, ny, permittivity.shape[0], norm)
        f32 = jnp.float32
        hbm_spec = pl.BlockSpec(memory_space=pltpu.HBM)
        vmem_spec = pl.BlockSpec(memory_space=pltpu.VMEM)
        block = (3, nz, nx, ny)
        g, h, grad = pl.pallas_call(
            functools.partial(kernel, dims),
            out_shape=(
                pltpu.VMEM(block, f32), pltpu.VMEM(block, f32), pltpu.VMEM((1, NI), f32),
            ),
            in_specs=[hbm_spec] * 6 + [pl.BlockSpec(memory_space=pltpu.SMEM)],
            out_specs=(vmem_spec,) * 3,
            scratch_shapes=[
                pltpu.VMEM((4,) + block, f32),
                pltpu.VMEM((2,) + block, f32),
                pltpu.VMEM((4,) + block, f32),
                pltpu.VMEM((3,) + block, f32),
                pltpu.VMEM(block, f32),
                pltpu.VMEM((nz, nx, ny), jnp.int32),
                pltpu.VMEM((nz, nx, ny), jnp.int32),
                pltpu.VMEM((nz, nx, ny), f32),
                pltpu.VMEM((nz, nx, ny), f32),
                pltpu.VMEM((4, 2 * nz, ny), f32),
                pltpu.VMEM((4, 2 * nz, ny), f32),
                pltpu.VMEM((4, 1, ny), f32),
                pltpu.VMEM((4, 1, ny), f32),
                pltpu.VMEM((4, 2 * nz, ny), f32),
                pltpu.VMEM((4, 2, nx, ny), f32),
                pltpu.VMEM((4, 2 * nz, ny), f32),
                pltpu.VMEM((4, 2, nx, ny), f32),
                pltpu.VMEM((4, 1, ny), f32),
                pltpu.VMEM((4, 1, ny), f32),
                pltpu.VMEM((1, 1, 128), f32),
                pltpu.VMEM((n_x * n_z, 1, 128), f32),
                pltpu.SemaphoreType.DMA((6, nz)),
                pltpu.SemaphoreType.DMA((4, 6)),
                pltpu.SemaphoreType.DMA((4, 6)),
                pltpu.SemaphoreType.DMA,
                pltpu.SemaphoreType.DMA,
            ],
            compiler_params=pltpu.CompilerParams(
                collective_id=0, has_side_effects=True
            ),
            name="yee_adjoint",
        )(e_check, h_check, adj_e, adj_h, material, owner, permittivity)
        g, h, grad = pl.pallas_call(
            store,
            out_shape=(
                jax.ShapeDtypeStruct(e_check.shape, f32),
                jax.ShapeDtypeStruct(e_check.shape, f32),
                jax.ShapeDtypeStruct((1, NI), f32),
            ),
            in_specs=[vmem_spec] * 3,
            out_specs=(hbm_spec,) * 3,
            scratch_shapes=[pltpu.SemaphoreType.DMA((3, nz))],
            compiler_params=pltpu.CompilerParams(vmem_limit_bytes=2**20),
            name="store_outputs",
        )(g, h, grad)
        return g, h, grad.reshape(NI)

    split = P(None, "xy", "gz", None)
    return jax.shard_map(
        body,
        mesh=mesh,
        in_specs=(split,) * 4 + (P("xy", "gz", None),) * 2 + (P(),),
        out_specs=(split, split, P()),
        check_vma=False,
    )
```
